32 devices in a mesh: dp: 4 (over x, core), band: 8 (over z, y).
Axes of the slice: x: 2, y: 2, z: 4, core: 2. Of those that a mesh axis runs over, the one named last changes fastest.
Arguments:
- features: bfloat16 [8160, 256], P(('dp', 'band')), parts along dimension 0, may hold values from -6 to 6
- corners: int32 [8160, 512], P(('dp', 'band')), parts along dimension 0, may hold values from 0 to 1535, as said below
- bilinear: float32 [8160, 512], P(('dp', 'band')), parts along dimension 0, may hold values from 0.08 to 0.5, as said below
- attention: float32 [8160, 128], P(('dp', 'band')), parts along dimension 0, may hold values from 0 to 1, as said below
- w_value: bfloat16 [256, 256], replicated, may hold values from -0.375 to 0.375
- b_value: float32 [256], replicated, may hold values from -0.6 to 0.6
- w_out: bfloat16 [256, 256], replicated, may hold values from -1.5 to 1.5
- b_out: float32 [256], replicated, may hold values from -3 to 3
- norm1_gain: float32 [256], replicated, may hold values from 0.5 to 1.5
- norm1_bias: float32 [256], replicated, may hold values from -3 to 3
- w_in: bfloat16 [256, 1024], replicated, may hold values from -0.375 to 0.375
- b_in: float32 [1024], replicated, may hold values from -3 to 3
- w_ffout: bfloat16 [1024, 256], replicated, may hold values from -0.1875 to 0.1875
- b_ffout: float32 [256], replicated, may hold values from -3 to 3
- norm2_gain: float32 [256], replicated, may hold values from 0.5 to 1.5
- norm2_bias: float32 [256], replicated, may hold values from -3 to 3
Outputs:
- encoded: bfloat16 [8160, 256], P(('dp', 'band')), parts along dimension 0
The draws below stay inside these ranges and needn't reach their ends.
There are 4 independent parts, one for each index of `dp`. The reference program is written for one: setup_inputs(seed, part) draws one part's arguments, and reference() takes and returns one part's arrays. A program takes and returns all parts, laid end to end along the dimension named above; an argument that names none is the same for every part. Nothing has to cross between parts.
Inputs may be any that keep to these rules, and one draw needn't show every extreme that they name: An entry for level l is a row of a map of 192 * 8 // 4**l tokens laid out in rows of 128 // 2**l; the four corners of a point are k, k + 1, k + 128 // 2**l and k + 128 // 2**l + 1 in that order. `bilinear`: the four corner weights of a point are positive and sum to one. `attention`: for each token and head the 16 weights are positive and sum to one.
All inputs are finite; a program needn't handle non-finite values.
Results may differ from the reference program's by a relative error of at most 0.009.
Values may be sent and summed in bfloat16 or wider, within the bound.
A program may use at most 64 MiB of HBM per device.

```python
import jax
import jax.numpy as jnp
from jax import lax

D = 256
HEADS = 8
FF = 1024
LEVELS = 4
POINTS = 4
MAP_W = 128
ROWS_DEV = 192
BAND_ROWS = 255
TOKENS = 2040


def query_place():
    band_total = TOKENS // BAND_ROWS
    token_ids = jnp.arange(TOKENS, dtype=jnp.int32)
    band_index = token_ids // BAND_ROWS
    local_row = token_ids % BAND_ROWS
    own_position = band_index * ROWS_DEV + local_row
    own_length = jnp.zeros((TOKENS,), jnp.int32) + ROWS_DEV * band_total
    offset_rows = 0
    for level_index in range(LEVELS):
        rows_here = ROWS_DEV // 4 ** level_index
        inside = (local_row >= offset_rows) & (local_row < offset_rows + rows_here)
        own_position = jnp.where(inside, band_index * rows_here + local_row - offset_rows, own_position)
        own_length = jnp.where(inside, rows_here * band_total, own_length)
        offset_rows = offset_rows + rows_here
    return (own_position, own_length)


def draw_corners(key, part):
    band_total = TOKENS // BAND_ROWS
    own_position, own_length = query_place()
    tables = []
    for level_index in range(LEVELS):
        rows_here = ROWS_DEV // 4 ** level_index
        length = rows_here * band_total
        stride = MAP_W // 2 ** level_index
        shape_here = (TOKENS, HEADS, POINTS)
        keys_here = jax.random.split(jax.random.fold_in(key, 11 + level_index), 4)
        centre = (own_position * length // own_length)[:, None, None]
        jitter = jax.random.randint(keys_here[0], shape_here, -rows_here, rows_here + 1) + jax.random.randint(keys_here[1], shape_here, -rows_here, rows_here + 1)
        faraway = jax.random.randint(keys_here[2], shape_here, 0, length)
        choose = jax.random.randint(keys_here[3], shape_here, 0, 4) != 0
        anchor = jnp.clip(jnp.where(choose, faraway, centre + jitter), 0, length - stride - 2)
        tables.append(jnp.stack([anchor, anchor + 1, anchor + stride, anchor + stride + 1], axis=-1))
    return jnp.stack(tables, axis=2).reshape(TOKENS, HEADS * LEVELS * POINTS * 4).astype(jnp.int32)


def draw_bilinear(key, part):
    key_first, key_second = jax.random.split(jax.random.fold_in(key, 29))
    shape_here = (TOKENS, HEADS * LEVELS * POINTS)
    first = jax.random.uniform(key_first, shape_here, jnp.float32)
    second = jax.random.uniform(key_second, shape_here, jnp.float32)
    first = 0.3 + 0.4 * first
    second = 0.3 + 0.4 * second
    stacked = jnp.stack([(1.0 - first) * (1.0 - second), first * (1.0 - second), (1.0 - first) * second, first * second], axis=-1)
    return stacked.reshape(TOKENS, HEADS * LEVELS * POINTS * 4).astype(jnp.float32)


def draw_attention(key, part):
    key_logit = jax.random.fold_in(key, 37)
    shape_here = (TOKENS, HEADS, LEVELS * POINTS)
    finer = jnp.arange(LEVELS * POINTS, dtype=jnp.int32) // POINTS < 2
    noise = jax.random.normal(key_logit, shape_here, jnp.float32)
    logits = jnp.where(finer, 0.3 * noise, 1.35 + 0.8 * noise)
    return jax.nn.softmax(logits, axis=-1).reshape(TOKENS, HEADS * LEVELS * POINTS).astype(jnp.float32)


def block_scale(stream_key, shape, pieces, smallest, top_value):
    def one(axis_at, shards_of):
        steps = jax.random.uniform(jax.random.fold_in(jax.random.fold_in(stream_key, 6), axis_at), (shards_of,), jnp.float32, smallest / len(pieces), top_value / len(pieces))
        return jnp.repeat(jnp.exp(steps), shape[axis_at] // shards_of).reshape((-1,) + (1,) * (len(shape) - axis_at - 1))

    level = one(*pieces[0])
    for cut in pieces[1:]:
        level = level * one(*cut)
    return level


def bell_draw(rng, dims, deviation, limit, pieces=(), held_as=jnp.bfloat16):
    loudness = block_scale(rng, dims, pieces, -0.22, 0.18) if pieces else 1.0
    values = jax.random.normal(rng, dims, jnp.float32) * deviation * loudness
    return jnp.minimum(jnp.maximum(values, -limit), limit).astype(held_as)


def setup_inputs(seed: int = 0, part: int = 0) -> dict:
    key_list = jax.random.split(jax.random.key(seed), 17)
    own_keys = jax.random.split(jax.random.fold_in(key_list[16], part), 17)
    return {
        "features": bell_draw(own_keys[0], (TOKENS, D), 1.0, 6.0, ((0, 8),)),
        "corners": draw_corners(jax.random.fold_in(jax.random.fold_in(key_list[16], part), 71), part),
        "bilinear": draw_bilinear(jax.random.fold_in(jax.random.fold_in(key_list[16], part), 71), part),
        "attention": draw_attention(jax.random.fold_in(jax.random.fold_in(key_list[16], part), 71), part),
        "w_value": bell_draw(key_list[4], (D, D), D ** -0.5, 0.375),
        "b_value": bell_draw(key_list[5], (D,), 0.1, 0.6, (), jnp.float32),
        "w_out": bell_draw(key_list[6], (D, D), (D // 16) ** -0.5, 1.5),
        "b_out": bell_draw(key_list[7], (D,), 0.5, 3.0, (), jnp.float32),
        "norm1_gain": jnp.clip(1.0 + 0.1 * jax.random.normal(key_list[8], (D,), jnp.float32), 0.5, 1.5),
        "norm1_bias": bell_draw(key_list[9], (D,), 0.5, 3.0, (), jnp.float32),
        "w_in": bell_draw(key_list[10], (D, FF), D ** -0.5, 0.375),
        "b_in": bell_draw(key_list[11], (FF,), 0.5, 3.0, (), jnp.float32),
        "w_ffout": bell_draw(key_list[12], (FF, D), FF ** -0.5, 0.1875),
        "b_ffout": bell_draw(key_list[13], (D,), 0.5, 3.0, (), jnp.float32),
        "norm2_gain": jnp.clip(1.0 + 0.1 * jax.random.normal(key_list[14], (D,), jnp.float32), 0.5, 1.5),
        "norm2_bias": bell_draw(key_list[15], (D,), 0.5, 3.0, (), jnp.float32),
    }


def layer_norm(inputs, gain, shift):
    average = lax.optimization_barrier(jnp.mean(inputs, axis=-1, keepdims=True))
    centred = inputs - average
    variance = lax.optimization_barrier(jnp.mean(centred * centred, axis=-1, keepdims=True))
    return centred * lax.rsqrt(variance + 1e-05) * gain + shift

def reference(features, corners, bilinear, attention, w_value, b_value, w_out, b_out, norm1_gain, norm1_bias, w_in, b_in, w_ffout, b_ffout, norm2_gain, norm2_bias):
    token_count, model_width = features.shape
    head_dim = model_width // HEADS
    samples = LEVELS * POINTS * 4
    segment_rows = [ROWS_DEV // 4 ** level_index for level_index in range(LEVELS)]
    segment_start = [sum(segment_rows[:level_index]) for level_index in range(LEVELS)]
    value_rows = (jnp.dot(features, w_value, preferred_element_type=jnp.float32) + b_value).astype(jnp.bfloat16)
    weight = (attention.reshape(token_count, HEADS, LEVELS, POINTS, 1) * bilinear.reshape(token_count, HEADS, LEVELS, POINTS, 4)).astype(jnp.bfloat16)
    weight = weight.reshape(token_count, HEADS, samples)
    corner_table = corners.reshape(token_count, HEADS, LEVELS, POINTS * 4)
    places = []
    for level_index in range(LEVELS):
        level_corner = corner_table[:, :, level_index]
        places.append(level_corner // segment_rows[level_index] * BAND_ROWS + segment_start[level_index] + level_corner % segment_rows[level_index])
    place_table = jnp.stack(places, axis=2).reshape(token_count, HEADS, samples)
    flat_index = (place_table * HEADS + jnp.arange(HEADS, dtype=jnp.int32)[None, :, None]).astype(jnp.int32)
    flat_value = value_rows.reshape(token_count * HEADS, head_dim)
    band_count = token_count // BAND_ROWS

    def blend_block(block_args):
        index_block, weight_block = block_args
        picked = flat_value[index_block].astype(jnp.float32)
        return lax.optimization_barrier(jnp.sum(weight_block.astype(jnp.float32)[..., None] * picked, axis=2))
    sampled = lax.map(blend_block, (flat_index.reshape(band_count, BAND_ROWS, HEADS, samples), weight.reshape(band_count, BAND_ROWS, HEADS, samples)))
    sampled = sampled.reshape(token_count, model_width).astype(jnp.bfloat16)
    attended = jnp.dot(sampled, w_out, preferred_element_type=jnp.float32) + b_out
    middle = layer_norm(features.astype(jnp.float32) + attended, norm1_gain, norm1_bias).astype(jnp.bfloat16)
    hidden = jnp.maximum(jnp.dot(middle, w_in, preferred_element_type=jnp.float32) + b_in, 0.0).astype(jnp.bfloat16)
    result = middle.astype(jnp.float32) + jnp.dot(hidden, w_ffout, preferred_element_type=jnp.float32) + b_ffout
    return layer_norm(result, norm2_gain, norm2_bias).astype(jnp.bfloat16)
```

```python
import functools

import jax
import jax.numpy as jnp
from jax import lax
from jax.experimental import pallas as pl
from jax.experimental.pallas import tpu as pltpu
from jax.sharding import PartitionSpec as P

HEADS = 8
LEVELS = 4
POINTS = 4
ROWS_DEV = 192
MAP_W = 128
LANES = 128
STRIDE = LANES - 1

F32 = jnp.float32
BF16 = jnp.bfloat16
MESH = pl.DeviceIdType.MESH


def plan(bands):
    rows = [ROWS_DEV // 4**level for level in range(LEVELS)]
    starts = [sum(rows[:level]) for level in range(LEVELS)]
    widths = [MAP_W // 2**level for level in range(LEVELS)]
    lengths = [count * bands for count in rows]
    merged, used = {}, 0
    for level in reversed(range(LEVELS)):
        if used + lengths[level] <= LANES:
            merged[level] = used
            used += lengths[level]
        else:
            break
    windowed = [level for level in range(LEVELS) if level not in merged]
    groups = {level: (lengths[level] - widths[level] - 2) // STRIDE + 1 for level in windowed}
    return rows, starts, widths, lengths, merged, windowed, groups


def flat_lanes(length, width, groups):
    need = STRIDE * (groups - 1) + width + LANES
    return -(-max(length, need) // LANES) * LANES


def norm(inputs, gain, shift):
    average = jnp.mean(inputs, axis=-1, keepdims=True)
    centred = inputs - average
    variance = jnp.mean(centred * centred, axis=-1, keepdims=True)
    return centred * lax.rsqrt(variance + 1e-05) * gain + shift


def one_hot_pair(iota, place, weights):
    low = iota == place
    high = iota == place + 1.0
    zero = jnp.zeros((), F32)
    top = jnp.where(low, weights[0], jnp.where(high, weights[1], zero))
    bottom = jnp.where(low, weights[2], jnp.where(high, weights[3], zero))
    return top, bottom


def kernel(
    bands,
    feat,
    corners,
    bilinear,
    attention,
    w_value,
    b_value,
    w_out_hbm,
    b_out,
    gain1,
    bias1,
    w_in_hbm,
    b_in,
    w_ff_hbm,
    b_ff,
    gain2,
    bias2,
    out,
    gathered,
    place_t,
    group_t,
    bil_t,
    att_t,
    hot,
    hot_merged,
    table_merged,
    samp_t,
    w_out,
    w_in,
    w_ff,
    send_sem,
    recv_sem,
    load_sem,
    *level_scratch,
):
    rows, starts, widths, lengths, merged, windowed, groups = plan(bands)
    flats = level_scratch[:LEVELS]
    tables = dict(zip(windowed, level_scratch[LEVELS:]))
    tokens, model = feat.shape
    head_dim = model // HEADS
    padded = place_t.shape[1]
    me = lax.axis_index("band")

    loads = [
        pltpu.make_async_copy(source, target, load_sem.at[number])
        for number, (source, target) in enumerate(
            ((w_out_hbm, w_out), (w_in_hbm, w_in), (w_ff_hbm, w_ff))
        )
    ]
    for load in loads:
        load.start()

    barrier = pltpu.get_barrier_semaphore()
    for offset in range(1, bands):
        pl.semaphore_signal(
            barrier, inc=1, device_id={"band": lax.rem(me + offset, bands)}, device_id_type=MESH
        )
    pl.semaphore_wait(barrier, bands - 1)

    def send(offset):
        return pltpu.make_async_remote_copy(
            src_ref=feat,
            dst_ref=gathered.at[me],
            send_sem=send_sem.at[offset],
            recv_sem=recv_sem.at[me],
            device_id={"band": lax.rem(me + offset, bands)},
            device_id_type=MESH,
        )

    for offset in range(1, bands):
        send(offset).start()

    gathered[me] = feat[...]

    def turned(block):
        tail = jnp.zeros((padded - tokens, block.shape[1]), F32)
        return jnp.transpose(jnp.concatenate([block, tail], axis=0))

    corner_t = turned(corners[...].astype(F32))
    group_t[...] = jnp.floor((corner_t + 0.5) * (1.0 / STRIDE))
    place_t[...] = corner_t
    bil_t[...] = turned(bilinear[...])
    att_t[...] = turned(attention[...])
    for level in range(LEVELS):
        flats[level][...] = jnp.zeros(flats[level].shape, F32)

    iota = lax.broadcasted_iota(jnp.int32, (LANES, padded), 0).astype(F32)

    def point_weights(point):
        share = att_t[pl.ds(point, 1), :]
        return [
            (share * bil_t[pl.ds(point * 4 + corner, 1), :]).astype(BF16).astype(F32)
            for corner in range(4)
        ]

    def build(head, carry):
        for slot, level in enumerate(windowed):
            for which in range(POINTS):
                point = (head * LEVELS + level) * POINTS + which
                place = place_t[pl.ds(point * 4, 1), :] - STRIDE * group_t[pl.ds(point * 4, 1), :]
                top, bottom = one_hot_pair(iota, place, point_weights(point))
                hot[head, slot * POINTS + which, 0:LANES, :] = top.astype(BF16)
                hot[head, slot * POINTS + which, LANES:, :] = bottom.astype(BF16)
        top_sum = jnp.zeros((LANES, padded), F32)
        bottom_sum = jnp.zeros((LANES, padded), F32)
        for level in merged:
            for which in range(POINTS):
                point = (head * LEVELS + level) * POINTS + which
                place = place_t[pl.ds(point * 4, 1), :] + float(merged[level])
                top, bottom = one_hot_pair(iota, place, point_weights(point))
                top_sum += top
                bottom_sum += bottom
        hot_merged[head, 0:LANES, :] = top_sum.astype(BF16)
        hot_merged[head, LANES:, :] = bottom_sum.astype(BF16)
        return carry

    lax.fori_loop(0, HEADS, build, 0)

    w_value_t = jnp.transpose(w_value[...].astype(F32)).astype(BF16)
    shift_t = jnp.transpose(jnp.broadcast_to(b_value[...], (LANES, model)))[:, 0:1]

    for offset in range(1, bands):
        copy = pltpu.make_async_remote_copy(
            src_ref=feat,
            dst_ref=gathered.at[lax.rem(me - offset + bands, bands)],
            send_sem=send_sem.at[offset],
            recv_sem=recv_sem.at[lax.rem(me - offset + bands, bands)],
            device_id={"band": lax.rem(me + offset, bands)},
            device_id_type=MESH,
        )
        copy.wait_recv()

    for band in range(bands):
        value_t = lax.dot_general(
            w_value_t, gathered[band], (((1,), (1,)), ((), ())), preferred_element_type=F32
        )
        value_t = (value_t + shift_t).astype(BF16).astype(F32)
        for level in range(LEVELS):
            count = rows[level]
            flats[level][:, band * count : (band + 1) * count] = value_t[
                :, starts[level] : starts[level] + count
            ]

    for level in windowed:
        for group in range(groups[level]):
            base = STRIDE * group
            top = flats[level][:, base : base + LANES].astype(BF16)
            under = base + widths[level]
            bottom = flats[level][:, under : under + LANES].astype(BF16)
            for head in range(HEADS):
                part = slice(head * head_dim, (head + 1) * head_dim)
                into = slice(group * head_dim, (group + 1) * head_dim)
                tables[level][head, into, 0:LANES] = top[part, :]
                tables[level][head, into, LANES:] = bottom[part, :]
    lane = lax.broadcasted_iota(jnp.int32, (1, LANES), 1)
    top = jnp.zeros((model, LANES), F32)
    bottom = jnp.zeros((model, LANES), F32)
    for level, begin in merged.items():
        inside = (lane >= begin) & (lane < begin + lengths[level])
        piece = flats[level][:, 0:LANES]
        top += jnp.where(inside, pltpu.roll(piece, begin, 1), 0.0)
        bottom += jnp.where(
            inside, pltpu.roll(piece, (begin - widths[level]) % LANES, 1), 0.0
        )
    for head in range(HEADS):
        part = slice(head * head_dim, (head + 1) * head_dim)
        table_merged[head, :, 0:LANES] = top[part, :].astype(BF16)
        table_merged[head, :, LANES:] = bottom[part, :].astype(BF16)

    def blend(head, carry):
        total = jnp.dot(table_merged[head], hot_merged[head], preferred_element_type=F32)
        for slot, level in enumerate(windowed):
            for which in range(POINTS):
                point = (head * LEVELS + level) * POINTS + which
                mine = group_t[pl.ds(point * 4, 1), :]
                picked = jnp.dot(
                    tables[level][head],
                    hot[head, slot * POINTS + which],
                    preferred_element_type=F32,
                )
                for group in range(groups[level]):
                    total += jnp.where(
                        mine == float(group),
                        picked[group * head_dim : (group + 1) * head_dim, :],
                        0.0,
                    )
        samp_t[pl.ds(pl.multiple_of(head * head_dim, head_dim), head_dim), :] = total
        return carry

    lax.fori_loop(0, HEADS, blend, 0)

    for load in loads:
        load.wait()
    sampled = jnp.transpose(samp_t[...])[0:tokens, :].astype(BF16)
    attended = jnp.dot(sampled, w_out[...], preferred_element_type=F32) + b_out[...]
    middle = norm(feat[...].astype(F32) + attended, gain1[...], bias1[...]).astype(BF16)
    hidden = jnp.maximum(
        jnp.dot(middle, w_in[...], preferred_element_type=F32) + b_in[...], 0.0
    ).astype(BF16)
    result = (
        middle.astype(F32)
        + jnp.dot(hidden, w_ff[...], preferred_element_type=F32)
        + b_ff[...]
    )
    out[...] = norm(result, gain2[...], bias2[...]).astype(BF16)
    for offset in range(1, bands):
        send(offset).wait_send()


def body(bands, *args):
    feat, corners = args[0], args[1]
    tokens, model = feat.shape
    padded = -(-tokens // LANES) * LANES
    rows, starts, widths, lengths, merged, windowed, groups = plan(bands)
    head_dim = model // HEADS
    samples = corners.shape[1]
    operands = [
        argument.reshape(1, -1) if argument.ndim == 1 else argument for argument in args
    ]
    anywhere = {6, 10, 12}
    specs = [
        pl.BlockSpec(memory_space=pl.ANY if number in anywhere else pltpu.VMEM)
        for number in range(len(operands))
    ]
    flat_shapes = [
        pltpu.VMEM(
            (model, flat_lanes(lengths[level], widths[level], groups.get(level, 1))), F32
        )
        for level in range(LEVELS)
    ]
    table_shapes = [
        pltpu.VMEM((HEADS, groups[level] * head_dim, 2 * LANES), BF16) for level in windowed
    ]
    scratch = [
        pltpu.VMEM((bands, tokens, model), BF16),
        pltpu.VMEM((samples, padded), F32),
        pltpu.VMEM((samples, padded), F32),
        pltpu.VMEM((samples, padded), F32),
        pltpu.VMEM((samples // 4, padded), F32),
        pltpu.VMEM((HEADS, len(windowed) * POINTS, 2 * LANES, padded), BF16),
        pltpu.VMEM((HEADS, 2 * LANES, padded), BF16),
        pltpu.VMEM((HEADS, head_dim, 2 * LANES), BF16),
        pltpu.VMEM((model, padded), F32),
        pltpu.VMEM(args[6].shape, BF16),
        pltpu.VMEM(args[10].shape, BF16),
        pltpu.VMEM(args[12].shape, BF16),
        pltpu.SemaphoreType.DMA((bands,)),
        pltpu.SemaphoreType.DMA((bands,)),
        pltpu.SemaphoreType.DMA((3,)),
    ] + flat_shapes + table_shapes
    return pl.pallas_call(
        functools.partial(kernel, bands),
        out_shape=jax.ShapeDtypeStruct((tokens, model), BF16),
        in_specs=specs,
        out_specs=pl.BlockSpec(memory_space=pltpu.VMEM),
        scratch_shapes=scratch,
        compiler_params=pltpu.CompilerParams(
            collective_id=0, has_side_effects=True, vmem_limit_bytes=60 * 1024 * 1024
        ),
        name="layer",
    )(*operands)


def solution(mesh):
    split = P(("dp", "band"), None)
    in_specs = (split,) * 4 + (P(),) * 12
    return jax.shard_map(
        functools.partial(body, mesh.shape["band"]),
        mesh=mesh,
        in_specs=in_specs,
        out_specs=split,
        check_vma=False,
    )
```

```python
import functools

import jax
import jax.numpy as jnp
from jax import lax
from jax.experimental import pallas as pl
from jax.experimental.pallas import tpu as pltpu
from jax.sharding import PartitionSpec as P

HEADS = 8
LEVELS = 4
POINTS = 4
ROWS_DEV = 192
MAP_W = 128
LANES = 128
STRIDE = LANES - 1
CHUNK = 128
BUILT = (3, 5, 7, 8)

F32 = jnp.float32
BF16 = jnp.bfloat16
MESH = pl.DeviceIdType.MESH


def plan(bands):
    rows = [ROWS_DEV // 4**level for level in range(LEVELS)]
    starts = [sum(rows[:level]) for level in range(LEVELS)]
    widths = [MAP_W // 2**level for level in range(LEVELS)]
    lengths = [count * bands for count in rows]
    merged, used = {}, 0
    for level in reversed(range(LEVELS)):
        if used + lengths[level] <= LANES:
            merged[level] = used
            used += lengths[level]
        else:
            break
    windowed = [level for level in range(LEVELS) if level not in merged]
    groups = {level: (lengths[level] - widths[level] - 2) // STRIDE + 1 for level in windowed}
    return rows, starts, widths, lengths, merged, windowed, groups


def flat_lanes(length, width, groups):
    need = STRIDE * (groups - 1) + width + LANES
    return -(-max(length, need) // LANES) * LANES


def norm(inputs, gain, shift):
    average = jnp.mean(inputs, axis=-1, keepdims=True)
    centred = inputs - average
    variance = jnp.mean(centred * centred, axis=-1, keepdims=True)
    return centred * lax.rsqrt(variance + 1e-05) * gain + shift


def one_hot_pair(iota, place, weights):
    low = iota == place
    high = iota == place + 1.0
    zero = jnp.zeros((), F32)
    top = jnp.where(low, weights[0], jnp.where(high, weights[1], zero))
    bottom = jnp.where(low, weights[2], jnp.where(high, weights[3], zero))
    return top, bottom


def kernel(
    bands,
    feat,
    corners_hbm,
    bilinear_hbm,
    attention_hbm,
    w_value_hbm,
    b_value,
    w_out_hbm,
    b_out,
    gain1,
    bias1,
    w_in_hbm,
    b_in,
    w_ff_hbm,
    b_ff,
    gain2,
    bias2,
    out,
    gathered,
    values,
    corners,
    bilinear,
    attention,
    w_value,
    w_value_t,
    shift_t,
    place_t,
    group_t,
    bil_t,
    att_t,
    hot,
    hot_merged,
    table_merged,
    samp_t,
    w_out,
    w_in,
    w_ff,
    send_sem,
    recv_sem,
    load_sem,
    *level_scratch,
):
    rows, starts, widths, lengths, merged, windowed, groups = plan(bands)
    flats = level_scratch[:LEVELS]
    tables = dict(zip(windowed, level_scratch[LEVELS:]))
    tokens, model = feat.shape
    head_dim = model // HEADS
    padded = place_t.shape[1]
    me = lax.axis_index("band")

    line = bands // 2
    mine_z, mine_y = me // 2, lax.rem(me, 2)
    partner = mine_z * 2 + 1 - mine_y
    has_left, has_right = mine_z > 0, mine_z < line - 1
    cuts = [(begin, min(begin + CHUNK, tokens) - begin) for begin in range(0, tokens, CHUNK)]

    sources = (corners_hbm, bilinear_hbm, attention_hbm, w_value_hbm, w_out_hbm, w_in_hbm, w_ff_hbm)
    targets = (corners, bilinear, attention, w_value, w_out, w_in, w_ff)
    loads = [
        pltpu.make_async_copy(source, target, load_sem.at[number])
        for number, (source, target) in enumerate(zip(sources, targets))
    ]

    barrier = pltpu.get_barrier_semaphore()

    def greet(target):
        pl.semaphore_signal(barrier, inc=1, device_id={"band": target}, device_id_type=MESH)

    greet(partner)
    pl.when(has_left)(lambda: greet(me - 2))
    pl.when(has_right)(lambda: greet(me + 2))
    pl.semaphore_wait(
        barrier, 1 + has_left.astype(jnp.int32) + has_right.astype(jnp.int32)
    )

    def copy_of(source, block, cut, target, lane):
        begin, count = cuts[cut]
        return pltpu.make_async_remote_copy(
            src_ref=source.at[pl.ds(begin, count)],
            dst_ref=gathered.at[block, pl.ds(begin, count)],
            send_sem=send_sem.at[lane, block, cut],
            recv_sem=recv_sem.at[block, cut],
            device_id={"band": target},
            device_id_type=MESH,
        )

    def moves(block, cut, source=None):
        source = gathered.at[block] if source is None else source
        left = copy_of(source, block, cut, me - 2, 0)
        right = copy_of(source, block, cut, me + 2, 1)
        across = copy_of(source, block, cut, partner, 2)
        return left, right, across

    for cut in range(len(cuts)):
        left, right, across = moves(me, cut, feat)
        pl.when(has_left)(left.start)
        pl.when(has_right)(right.start)
        across.start()
    for load in loads:
        load.start()

    def project(rows_in, block):
        value_t = lax.dot_general(
            w_value_t[...], rows_in, (((1,), (1,)), ((), ())), preferred_element_type=F32
        )
        values[block, :, 0:tokens] = (value_t + shift_t[:, 0:1]).astype(BF16).astype(F32)

    def stage(distance, cut):
        before, after = me - 2 * distance, me + 2 * distance

        @pl.when(mine_z >= distance)
        def _():
            left, right, across = moves(before, cut)
            across.wait_recv()
            pl.when(has_right)(right.start)
            across.start()

        @pl.when(mine_z + distance < line)
        def _():
            left, right, across = moves(after, cut)
            across.wait_recv()
            pl.when(has_left)(left.start)
            across.start()

        if cut == len(cuts) - 1:
            pl.when(mine_z >= distance)(lambda: project(gathered[before], before))
            pl.when(mine_z + distance < line)(lambda: project(gathered[after], after))

    def arrive(block):
        for cut in range(len(cuts)):
            moves(block, cut)[2].wait_recv()
        project(gathered[block], block)

    def finish(block, came_left, came_right, own=False):
        for cut in range(len(cuts)):
            left, right, across = moves(block, cut, feat if own else None)
            if own or came_right:
                pl.when(has_left)(left.wait_send)
            if own or came_left:
                pl.when(has_right)(right.wait_send)
            across.wait_send()

    for load in loads[:4]:
        load.wait()
    w_value_t[...] = jnp.transpose(w_value[...].astype(F32)).astype(BF16)
    shift_t[...] = jnp.transpose(jnp.broadcast_to(b_value[...], (LANES, model)))

    def turned(block):
        tail = jnp.zeros((padded - tokens, block.shape[1]), F32)
        return jnp.transpose(jnp.concatenate([block, tail], axis=0))

    corner_t = turned(corners[...].astype(F32))
    group_t[...] = jnp.floor((corner_t + 0.5) * (1.0 / STRIDE))
    place_t[...] = corner_t
    bil_t[...] = turned(bilinear[...])
    att_t[...] = turned(attention[...])
    for level in range(LEVELS):
        flats[level][...] = jnp.zeros(flats[level].shape, F32)

    iota = lax.broadcasted_iota(jnp.int32, (LANES, padded), 0).astype(F32)

    def point_weights(point):
        share = att_t[pl.ds(point, 1), :]
        return [
            (share * bil_t[pl.ds(point * 4 + corner, 1), :]).astype(BF16).astype(F32)
            for corner in range(4)
        ]

    def build(head, carry):
        for slot, level in enumerate(windowed):
            for which in range(POINTS):
                point = (head * LEVELS + level) * POINTS + which
                place = place_t[pl.ds(point * 4, 1), :] - STRIDE * group_t[pl.ds(point * 4, 1), :]
                top, bottom = one_hot_pair(iota, place, point_weights(point))
                hot[head, slot * POINTS + which, 0:LANES, :] = top.astype(BF16)
                hot[head, slot * POINTS + which, LANES:, :] = bottom.astype(BF16)
        top_sum = jnp.zeros((LANES, padded), F32)
        bottom_sum = jnp.zeros((LANES, padded), F32)
        for level in merged:
            for which in range(POINTS):
                point = (head * LEVELS + level) * POINTS + which
                place = place_t[pl.ds(point * 4, 1), :] + float(merged[level])
                top, bottom = one_hot_pair(iota, place, point_weights(point))
                top_sum += top
                bottom_sum += bottom
        hot_merged[head, 0:LANES, :] = top_sum.astype(BF16)
        hot_merged[head, LANES:, :] = bottom_sum.astype(BF16)
        return carry

    stages = [(distance, cut) for distance in range(1, line) for cut in range(len(cuts))]
    done = 0
    for number, entry in enumerate(stages):
        upto = min(HEADS, BUILT[min(number, len(BUILT) - 1)])
        if upto > done:
            lax.fori_loop(done, upto, build, 0)
            done = upto
        if number == 0:
            project(feat[...], me)
        stage(*entry)
    if done < HEADS:
        lax.fori_loop(done, HEADS, build, 0)
    arrive(partner)
    for distance in range(1, line):
        pl.when(mine_z >= distance)(functools.partial(arrive, partner - 2 * distance))
        pl.when(mine_z + distance < line)(functools.partial(arrive, partner + 2 * distance))

    for band in range(bands):
        value_t = values[band]
        for level in range(LEVELS):
            count = rows[level]
            flats[level][:, band * count : (band + 1) * count] = value_t[
                :, starts[level] : starts[level] + count
            ]

    for level in windowed:
        for group in range(groups[level]):
            base = STRIDE * group
            top = flats[level][:, base : base + LANES].astype(BF16)
            under = base + widths[level]
            bottom = flats[level][:, under : under + LANES].astype(BF16)
            for head in range(HEADS):
                part = slice(head * head_dim, (head + 1) * head_dim)
                into = slice(group * head_dim, (group + 1) * head_dim)
                tables[level][head, into, 0:LANES] = top[part, :]
                tables[level][head, into, LANES:] = bottom[part, :]
    lane = lax.broadcasted_iota(jnp.int32, (1, LANES), 1)
    top = jnp.zeros((model, LANES), F32)
    bottom = jnp.zeros((model, LANES), F32)
    for level, begin in merged.items():
        inside = (lane >= begin) & (lane < begin + lengths[level])
        piece = flats[level][:, 0:LANES]
        top += jnp.where(inside, pltpu.roll(piece, begin, 1), 0.0)
        bottom += jnp.where(
            inside, pltpu.roll(piece, (begin - widths[level]) % LANES, 1), 0.0
        )
    for head in range(HEADS):
        part = slice(head * head_dim, (head + 1) * head_dim)
        table_merged[head, :, 0:LANES] = top[part, :].astype(BF16)
        table_merged[head, :, LANES:] = bottom[part, :].astype(BF16)

    def blend(head, carry):
        total = jnp.dot(table_merged[head], hot_merged[head], preferred_element_type=F32)
        for slot, level in enumerate(windowed):
            for which in range(POINTS):
                point = (head * LEVELS + level) * POINTS + which
                mine = group_t[pl.ds(point * 4, 1), :]
                picked = jnp.dot(
                    tables[level][head],
                    hot[head, slot * POINTS + which],
                    preferred_element_type=F32,
                )
                for group in range(groups[level]):
                    total += jnp.where(
                        mine == float(group),
                        picked[group * head_dim : (group + 1) * head_dim, :],
                        0.0,
                    )
        samp_t[pl.ds(pl.multiple_of(head * head_dim, head_dim), head_dim), :] = total
        return carry

    lax.fori_loop(0, HEADS, blend, 0)

    for load in loads[4:]:
        load.wait()
    sampled = jnp.transpose(samp_t[...])[0:tokens, :].astype(BF16)
    attended = jnp.dot(sampled, w_out[...], preferred_element_type=F32) + b_out[...]
    middle = norm(feat[...].astype(F32) + attended, gain1[...], bias1[...]).astype(BF16)
    hidden = jnp.maximum(
        jnp.dot(middle, w_in[...], preferred_element_type=F32) + b_in[...], 0.0
    ).astype(BF16)
    result = (
        middle.astype(F32)
        + jnp.dot(hidden, w_ff[...], preferred_element_type=F32)
        + b_ff[...]
    )
    out[...] = norm(result, gain2[...], bias2[...]).astype(BF16)
    finish(me, False, False, own=True)
    for distance in range(1, line):
        pl.when(mine_z >= distance)(
            functools.partial(finish, me - 2 * distance, True, False)
        )
        pl.when(mine_z + distance < line)(
            functools.partial(finish, me + 2 * distance, False, True)
        )


def body(bands, *args):
    feat, corners = args[0], args[1]
    tokens, model = feat.shape
    padded = -(-tokens // LANES) * LANES
    rows, starts, widths, lengths, merged, windowed, groups = plan(bands)
    head_dim = model // HEADS
    samples = corners.shape[1]
    operands = [
        argument.reshape(1, -1) if argument.ndim == 1 else argument for argument in args
    ]
    anywhere = {1, 2, 3, 4, 6, 10, 12}
    cuts = -(-tokens // CHUNK)
    specs = [
        pl.BlockSpec(memory_space=pl.ANY if number in anywhere else pltpu.VMEM)
        for number in range(len(operands))
    ]
    flat_shapes = [
        pltpu.VMEM(
            (model, flat_lanes(lengths[level], widths[level], groups.get(level, 1))), F32
        )
        for level in range(LEVELS)
    ]
    table_shapes = [
        pltpu.VMEM((HEADS, groups[level] * head_dim, 2 * LANES), BF16) for level in windowed
    ]
    scratch = [
        pltpu.VMEM((bands, tokens, model), BF16),
        pltpu.VMEM((bands, model, padded), F32),
        pltpu.VMEM(args[1].shape, jnp.int32),
        pltpu.VMEM(args[2].shape, F32),
        pltpu.VMEM(args[3].shape, F32),
        pltpu.VMEM(args[4].shape, BF16),
        pltpu.VMEM(args[4].shape, BF16),
        pltpu.VMEM((model, LANES), F32),
        pltpu.VMEM((samples, padded), F32),
        pltpu.VMEM((samples, padded), F32),
        pltpu.VMEM((samples, padded), F32),
        pltpu.VMEM((samples // 4, padded), F32),
        pltpu.VMEM((HEADS, len(windowed) * POINTS, 2 * LANES, padded), BF16),
        pltpu.VMEM((HEADS, 2 * LANES, padded), BF16),
        pltpu.VMEM((HEADS, head_dim, 2 * LANES), BF16),
        pltpu.VMEM((model, padded), F32),
        pltpu.VMEM(args[6].shape, BF16),
        pltpu.VMEM(args[10].shape, BF16),
        pltpu.VMEM(args[12].shape, BF16),
        pltpu.SemaphoreType.DMA((3, bands, cuts)),
        pltpu.SemaphoreType.DMA((bands, cuts)),
        pltpu.SemaphoreType.DMA((len(anywhere),)),
    ] + flat_shapes + table_shapes
    return pl.pallas_call(
        functools.partial(kernel, bands),
        out_shape=jax.ShapeDtypeStruct((tokens, model), BF16),
        in_specs=specs,
        out_specs=pl.BlockSpec(memory_space=pltpu.VMEM),
        scratch_shapes=scratch,
        compiler_params=pltpu.CompilerParams(
            collective_id=0, has_side_effects=True, vmem_limit_bytes=60 * 1024 * 1024
        ),
        name="layer",
    )(*operands)


def solution(mesh):
    split = P(("dp", "band"), None)
    in_specs = (split,) * 4 + (P(),) * 12
    return jax.shard_map(
        functools.partial(body, mesh.shape["band"]),
        mesh=mesh,
        in_specs=in_specs,
        out_specs=split,
        check_vma=False,
    )
```

```python
import functools
import math

import jax
import jax.numpy as jnp
from jax import lax
from jax.experimental import pallas as pl
from jax.experimental.pallas import tpu as pltpu
from jax.sharding import PartitionSpec as P

HEADS = 8
LEVELS = 4
POINTS = 4
ROWS_DEV = 192
MAP_W = 128
LANES = 128
STRIDE = LANES - 1
CHUNK = 64
BUILT = (1, 2, 3, 4, 5, 6, 7, 8)

F32 = jnp.float32
BF16 = jnp.bfloat16
MESH = pl.DeviceIdType.MESH


def plan(bands):
    rows = [ROWS_DEV // 4**level for level in range(LEVELS)]
    starts = [sum(rows[:level]) for level in range(LEVELS)]
    widths = [MAP_W // 2**level for level in range(LEVELS)]
    lengths = [count * bands for count in rows]
    merged, used = {}, 0
    for level in reversed(range(LEVELS)):
        if used + lengths[level] <= LANES:
            merged[level] = used
            used += lengths[level]
        else:
            break
    windowed = [level for level in range(LEVELS) if level not in merged]
    groups = {level: (lengths[level] - widths[level] - 2) // STRIDE + 1 for level in windowed}
    return rows, starts, widths, lengths, merged, windowed, groups


def flat_lanes(length, width, groups):
    need = STRIDE * (groups - 1) + width + LANES
    return -(-max(length, need) // LANES) * LANES


def norm(inputs, gain, shift):
    average = jnp.mean(inputs, axis=-1, keepdims=True)
    centred = inputs - average
    variance = jnp.mean(centred * centred, axis=-1, keepdims=True)
    return centred * lax.rsqrt(variance + 1e-05) * gain + shift


def one_hot_pair(iota, place, weights):
    low = iota == place
    high = iota == place + 1.0
    zero = jnp.zeros((), F32)
    top = jnp.where(low, weights[0], jnp.where(high, weights[1], zero))
    bottom = jnp.where(low, weights[2], jnp.where(high, weights[3], zero))
    return top, bottom


def kernel(
    bands,
    feat,
    corners_hbm,
    bilinear_hbm,
    attention_hbm,
    w_value_hbm,
    b_value,
    out,
    gathered,
    values,
    corners,
    bilinear,
    attention,
    w_value,
    w_value_t,
    shift_t,
    place_t,
    group_t,
    bil_t,
    att_t,
    hot,
    hot_merged,
    table_merged,
    samp_t,
    send_sem,
    recv_sem,
    load_sem,
    *level_scratch,
):
    rows, starts, widths, lengths, merged, windowed, groups = plan(bands)
    flats = level_scratch[:LEVELS]
    tables = dict(zip(windowed, level_scratch[LEVELS:]))
    tokens, model = feat.shape
    head_dim = model // HEADS
    padded = place_t.shape[1]
    me = lax.axis_index("band")

    line = bands // 2
    mine_z, mine_y = me // 2, lax.rem(me, 2)
    partner = mine_z * 2 + 1 - mine_y
    has_left, has_right = mine_z > 0, mine_z < line - 1
    cuts = [(begin, min(begin + CHUNK, tokens) - begin) for begin in range(0, tokens, CHUNK)]

    sources = (corners_hbm, bilinear_hbm, attention_hbm, w_value_hbm)
    targets = (corners, bilinear, attention, w_value)
    loads = [
        pltpu.make_async_copy(source, target, load_sem.at[number])
        for number, (source, target) in enumerate(zip(sources, targets))
    ]

    barrier = pltpu.get_barrier_semaphore()

    def greet(target):
        pl.semaphore_signal(barrier, inc=1, device_id={"band": target}, device_id_type=MESH)

    greet(partner)
    pl.when(has_left)(lambda: greet(me - 2))
    pl.when(has_right)(lambda: greet(me + 2))
    pl.semaphore_wait(
        barrier, 1 + has_left.astype(jnp.int32) + has_right.astype(jnp.int32)
    )

    def copy_of(source, block, cut, target, lane):
        begin, count = cuts[cut]
        return pltpu.make_async_remote_copy(
            src_ref=source.at[pl.ds(begin, count)],
            dst_ref=gathered.at[block, pl.ds(begin, count)],
            send_sem=send_sem.at[lane, block, cut],
            recv_sem=recv_sem.at[block, cut],
            device_id={"band": target},
            device_id_type=MESH,
        )

    def moves(block, cut, source=None):
        source = gathered.at[block] if source is None else source
        left = copy_of(source, block, cut, me - 2, 0)
        right = copy_of(source, block, cut, me + 2, 1)
        across = copy_of(source, block, cut, partner, 2)
        return left, right, across

    for cut in range(len(cuts)):
        left, right, across = moves(me, cut, feat)
        pl.when(has_left)(left.start)
        pl.when(has_right)(right.start)
        across.start()
    for load in loads:
        load.start()

    def project(rows_in, block):
        value_t = lax.dot_general(
            w_value_t[...], rows_in, (((1,), (1,)), ((), ())), preferred_element_type=F32
        )
        values[block, :, 0:tokens] = (value_t + shift_t[:, 0:1]).astype(BF16).astype(F32)

    def stage(distance, cut):
        before, after = me - 2 * distance, me + 2 * distance

        @pl.when(mine_z >= distance)
        def _():
            left, right, across = moves(before, cut)
            across.wait_recv()
            pl.when(has_right)(right.start)
            across.start()

        @pl.when(mine_z + distance < line)
        def _():
            left, right, across = moves(after, cut)
            across.wait_recv()
            pl.when(has_left)(left.start)
            across.start()

        if cut == len(cuts) - 1:
            pl.when(mine_z >= distance)(lambda: project(gathered[before], before))
            pl.when(mine_z + distance < line)(lambda: project(gathered[after], after))

    def arrive(block):
        for cut in range(len(cuts)):
            moves(block, cut)[2].wait_recv()
        project(gathered[block], block)

    def finish(block, came_left, came_right, own=False):
        for cut in range(len(cuts)):
            left, right, across = moves(block, cut, feat if own else None)
            if own or came_right:
                pl.when(has_left)(left.wait_send)
            if own or came_left:
                pl.when(has_right)(right.wait_send)
            across.wait_send()

    for load in loads:
        load.wait()
    w_value_t[...] = jnp.transpose(w_value[...].astype(F32)).astype(BF16)
    shift_t[...] = jnp.transpose(jnp.broadcast_to(b_value[...], (LANES, model)))

    def turned(block):
        tail = jnp.zeros((padded - tokens, block.shape[1]), F32)
        return jnp.transpose(jnp.concatenate([block, tail], axis=0))

    corner_t = turned(corners[...].astype(F32))
    group_t[...] = jnp.floor((corner_t + 0.5) * (1.0 / STRIDE))
    place_t[...] = corner_t
    bil_t[...] = turned(bilinear[...])
    att_t[...] = turned(attention[...])
    for level in range(LEVELS):
        flats[level][...] = jnp.zeros(flats[level].shape, F32)

    iota = lax.broadcasted_iota(jnp.int32, (LANES, padded), 0).astype(F32)

    def point_weights(point):
        share = att_t[pl.ds(point, 1), :]
        return [
            (share * bil_t[pl.ds(point * 4 + corner, 1), :]).astype(BF16).astype(F32)
            for corner in range(4)
        ]

    def build(head, carry):
        for slot, level in enumerate(windowed):
            for which in range(POINTS):
                point = (head * LEVELS + level) * POINTS + which
                place = place_t[pl.ds(point * 4, 1), :] - STRIDE * group_t[pl.ds(point * 4, 1), :]
                top, bottom = one_hot_pair(iota, place, point_weights(point))
                hot[head, slot * POINTS + which, 0:LANES, :] = top.astype(BF16)
                hot[head, slot * POINTS + which, LANES:, :] = bottom.astype(BF16)
        top_sum = jnp.zeros((LANES, padded), F32)
        bottom_sum = jnp.zeros((LANES, padded), F32)
        for level in merged:
            for which in range(POINTS):
                point = (head * LEVELS + level) * POINTS + which
                place = place_t[pl.ds(point * 4, 1), :] + float(merged[level])
                top, bottom = one_hot_pair(iota, place, point_weights(point))
                top_sum += top
                bottom_sum += bottom
        hot_merged[head, 0:LANES, :] = top_sum.astype(BF16)
        hot_merged[head, LANES:, :] = bottom_sum.astype(BF16)
        return carry

    stages = [(distance, cut) for distance in range(1, line) for cut in range(len(cuts))]
    done = 0
    for number, entry in enumerate(stages):
        upto = min(HEADS, BUILT[min(number, len(BUILT) - 1)])
        if upto > done:
            lax.fori_loop(done, upto, build, 0)
            done = upto
        if number == 0:
            project(feat[...], me)
        stage(*entry)
    if done < HEADS:
        lax.fori_loop(done, HEADS, build, 0)
    arrive(partner)
    for distance in range(1, line):
        pl.when(mine_z >= distance)(functools.partial(arrive, partner - 2 * distance))
        pl.when(mine_z + distance < line)(functools.partial(arrive, partner + 2 * distance))

    for band in range(bands):
        value_t = values[band]
        for level in range(LEVELS):
            count = rows[level]
            flats[level][:, band * count : (band + 1) * count] = value_t[
                :, starts[level] : starts[level] + count
            ]

    for level in windowed:
        for group in range(groups[level]):
            base = STRIDE * group
            top = flats[level][:, base : base + LANES].astype(BF16)
            under = base + widths[level]
            bottom = flats[level][:, under : under + LANES].astype(BF16)
            for head in range(HEADS):
                part = slice(head * head_dim, (head + 1) * head_dim)
                into = slice(group * head_dim, (group + 1) * head_dim)
                tables[level][head, into, 0:LANES] = top[part, :]
                tables[level][head, into, LANES:] = bottom[part, :]
    lane = lax.broadcasted_iota(jnp.int32, (1, LANES), 1)
    top = jnp.zeros((model, LANES), F32)
    bottom = jnp.zeros((model, LANES), F32)
    for level, begin in merged.items():
        inside = (lane >= begin) & (lane < begin + lengths[level])
        piece = flats[level][:, 0:LANES]
        top += jnp.where(inside, pltpu.roll(piece, begin, 1), 0.0)
        bottom += jnp.where(
            inside, pltpu.roll(piece, (begin - widths[level]) % LANES, 1), 0.0
        )
    for head in range(HEADS):
        part = slice(head * head_dim, (head + 1) * head_dim)
        table_merged[head, :, 0:LANES] = top[part, :].astype(BF16)
        table_merged[head, :, LANES:] = bottom[part, :].astype(BF16)

    def blend(head, carry):
        total = jnp.dot(table_merged[head], hot_merged[head], preferred_element_type=F32)
        for slot, level in enumerate(windowed):
            for which in range(POINTS):
                point = (head * LEVELS + level) * POINTS + which
                mine = group_t[pl.ds(point * 4, 1), :]
                picked = jnp.dot(
                    tables[level][head],
                    hot[head, slot * POINTS + which],
                    preferred_element_type=F32,
                )
                for group in range(groups[level]):
                    total += jnp.where(
                        mine == float(group),
                        picked[group * head_dim : (group + 1) * head_dim, :],
                        0.0,
                    )
        samp_t[pl.ds(pl.multiple_of(head * head_dim, head_dim), head_dim), :] = total
        return carry

    lax.fori_loop(0, HEADS, blend, 0)

    out[...] = jnp.transpose(samp_t[...])[0:tokens, :].astype(BF16)
    finish(me, False, False, own=True)
    for distance in range(1, line):
        pl.when(mine_z >= distance)(
            functools.partial(finish, me - 2 * distance, True, False)
        )
        pl.when(mine_z + distance < line)(
            functools.partial(finish, me + 2 * distance, False, True)
        )


def tail(
    feat, sampled, w_out, b_out, gain1, bias1, w_in, b_in, w_ff, b_ff, gain2, bias2, out
):
    attended = jnp.dot(sampled[...], w_out[...], preferred_element_type=F32) + b_out[...]
    middle = norm(feat[...].astype(F32) + attended, gain1[...], bias1[...]).astype(BF16)
    hidden = jnp.maximum(
        jnp.dot(middle, w_in[...], preferred_element_type=F32) + b_in[...], 0.0
    ).astype(BF16)
    result = (
        middle.astype(F32)
        + jnp.dot(hidden, w_ff[...], preferred_element_type=F32)
        + b_ff[...]
    )
    out[...] = norm(result, gain2[...], bias2[...]).astype(BF16)


def body(bands, *args):
    feat, corners = args[0], args[1]
    tokens, model = feat.shape
    padded = -(-tokens // LANES) * LANES
    rows, starts, widths, lengths, merged, windowed, groups = plan(bands)
    head_dim = model // HEADS
    samples = corners.shape[1]
    operands = [
        argument.reshape(1, -1) if argument.ndim == 1 else argument for argument in args
    ]
    anywhere = {1, 2, 3, 4}
    cuts = -(-tokens // CHUNK)
    specs = [
        pl.BlockSpec(memory_space=pltpu.HBM if number in anywhere else pltpu.VMEM)
        for number in range(6)
    ]
    flat_shapes = [
        pltpu.VMEM(
            (model, flat_lanes(lengths[level], widths[level], groups.get(level, 1))), F32
        )
        for level in range(LEVELS)
    ]
    table_shapes = [
        pltpu.VMEM((HEADS, groups[level] * head_dim, 2 * LANES), BF16) for level in windowed
    ]
    scratch = [
        pltpu.VMEM((bands, tokens, model), BF16),
        pltpu.VMEM((bands, model, padded), F32),
        pltpu.VMEM(args[1].shape, jnp.int32),
        pltpu.VMEM(args[2].shape, F32),
        pltpu.VMEM(args[3].shape, F32),
        pltpu.VMEM(args[4].shape, BF16),
        pltpu.VMEM(args[4].shape, BF16),
        pltpu.VMEM((model, LANES), F32),
        pltpu.VMEM((samples, padded), F32),
        pltpu.VMEM((samples, padded), F32),
        pltpu.VMEM((samples, padded), F32),
        pltpu.VMEM((samples // 4, padded), F32),
        pltpu.VMEM((HEADS, len(windowed) * POINTS, 2 * LANES, padded), BF16),
        pltpu.VMEM((HEADS, 2 * LANES, padded), BF16),
        pltpu.VMEM((HEADS, head_dim, 2 * LANES), BF16),
        pltpu.VMEM((model, padded), F32),
        pltpu.SemaphoreType.DMA((3, bands, cuts)),
        pltpu.SemaphoreType.DMA((bands, cuts)),
        pltpu.SemaphoreType.DMA((len(anywhere),)),
    ] + flat_shapes + table_shapes
    held = sum(
        4 * math.prod(shape.shape) // (2 if shape.dtype == BF16 else 1)
        for shape in scratch
        if shape.memory_space == pltpu.VMEM
    )
    vmem = pl.BlockSpec(memory_space=pltpu.VMEM)
    sampled = pl.pallas_call(
        functools.partial(kernel, bands),
        out_shape=jax.ShapeDtypeStruct((tokens, model), BF16),
        in_specs=specs,
        out_specs=vmem,
        scratch_shapes=scratch,
        compiler_params=pltpu.CompilerParams(
            collective_id=0,
            has_side_effects=True,
            vmem_limit_bytes=min(held + 12 * 1024 * 1024, 60 * 1024 * 1024),
        ),
        name="sample",
    )(*operands[:6])
    return pl.pallas_call(
        tail,
        out_shape=jax.ShapeDtypeStruct((tokens, model), BF16),
        in_specs=[vmem] * 12,
        out_specs=vmem,
        compiler_params=pltpu.CompilerParams(vmem_limit_bytes=24 * 1024 * 1024),
        name="tail",
    )(operands[0], sampled, *operands[6:])


def solution(mesh):
    split = P(("dp", "band"), None)
    in_specs = (split,) * 4 + (P(),) * 12
    return jax.shard_map(
        functools.partial(body, mesh.shape["band"]),
        mesh=mesh,
        in_specs=in_specs,
        out_specs=split,
        check_vma=False,
    )
```

```python
import functools

import jax
import jax.numpy as jnp
from jax import lax
from jax.experimental import pallas as pl
from jax.experimental.pallas import tpu as pltpu
from jax.sharding import PartitionSpec as P

HEADS = 8
LEVELS = 4
POINTS = 4
ROWS_DEV = 192
MAP_W = 128
LANES = 128
STRIDE = LANES - 1
CHUNK = 64
BUILT = (1, 2, 3, 4, 5, 6, 7, 8)

F32 = jnp.float32
BF16 = jnp.bfloat16
MESH = pl.DeviceIdType.MESH


def plan(bands):
    rows = [ROWS_DEV // 4**level for level in range(LEVELS)]
    starts = [sum(rows[:level]) for level in range(LEVELS)]
    widths = [MAP_W // 2**level for level in range(LEVELS)]
    lengths = [count * bands for count in rows]
    merged, used = {}, 0
    for level in reversed(range(LEVELS)):
        if used + lengths[level] <= LANES:
            merged[level] = used
            used += lengths[level]
        else:
            break
    windowed = [level for level in range(LEVELS) if level not in merged]
    groups = {level: (lengths[level] - widths[level] - 2) // STRIDE + 1 for level in windowed}
    return rows, starts, widths, lengths, merged, windowed, groups


def flat_lanes(length, width, groups):
    need = STRIDE * (groups - 1) + width + LANES
    return -(-max(length, need) // LANES) * LANES


def norm(inputs, gain, shift):
    average = jnp.mean(inputs, axis=-1, keepdims=True)
    centred = inputs - average
    variance = jnp.mean(centred * centred, axis=-1, keepdims=True)
    return centred * lax.rsqrt(variance + 1e-05) * gain + shift


def one_hot_pair(iota, place, weights):
    low = iota == place
    high = iota == place + 1.0
    zero = jnp.zeros((), F32)
    top = jnp.where(low, weights[0], jnp.where(high, weights[1], zero))
    bottom = jnp.where(low, weights[2], jnp.where(high, weights[3], zero))
    return top, bottom


def kernel(
    bands,
    feat,
    corners_hbm,
    bilinear_hbm,
    attention_hbm,
    w_value_hbm,
    b_value,
    w_out_hbm,
    b_out,
    gain1,
    bias1,
    w_in_hbm,
    b_in,
    w_ff_hbm,
    b_ff,
    gain2,
    bias2,
    out,
    gathered,
    values,
    corners,
    bilinear,
    attention,
    w_value,
    w_value_t,
    shift_t,
    place_t,
    group_t,
    bil_t,
    att_t,
    hot,
    hot_merged,
    table_merged,
    samp_t,
    w_out,
    w_in,
    w_ff,
    send_sem,
    recv_sem,
    load_sem,
    *level_scratch,
):
    rows, starts, widths, lengths, merged, windowed, groups = plan(bands)
    flats = level_scratch[:LEVELS]
    tables = dict(zip(windowed, level_scratch[LEVELS:]))
    tokens, model = feat.shape
    head_dim = model // HEADS
    padded = place_t.shape[1]
    me = lax.axis_index("band")

    line = bands // 2
    mine_z, mine_y = me // 2, lax.rem(me, 2)
    partner = mine_z * 2 + 1 - mine_y
    has_left, has_right = mine_z > 0, mine_z < line - 1
    cuts = [(begin, min(begin + CHUNK, tokens) - begin) for begin in range(0, tokens, CHUNK)]

    sources = (corners_hbm, bilinear_hbm, attention_hbm, w_value_hbm, w_out_hbm, w_in_hbm, w_ff_hbm)
    targets = (corners, bilinear, attention, w_value, w_out, w_in, w_ff)
    loads = [
        pltpu.make_async_copy(source, target, load_sem.at[number])
        for number, (source, target) in enumerate(zip(sources, targets))
    ]

    barrier = pltpu.get_barrier_semaphore()

    def greet(target):
        pl.semaphore_signal(barrier, inc=1, device_id={"band": target}, device_id_type=MESH)

    greet(partner)
    pl.when(has_left)(lambda: greet(me - 2))
    pl.when(has_right)(lambda: greet(me + 2))
    pl.semaphore_wait(
        barrier, 1 + has_left.astype(jnp.int32) + has_right.astype(jnp.int32)
    )

    def copy_of(source, block, cut, target, lane):
        begin, count = cuts[cut]
        return pltpu.make_async_remote_copy(
            src_ref=source.at[pl.ds(begin, count)],
            dst_ref=gathered.at[block, pl.ds(begin, count)],
            send_sem=send_sem.at[lane, block, cut],
            recv_sem=recv_sem.at[block, cut],
            device_id={"band": target},
            device_id_type=MESH,
        )

    def moves(block, cut, source=None):
        source = gathered.at[block] if source is None else source
        left = copy_of(source, block, cut, me - 2, 0)
        right = copy_of(source, block, cut, me + 2, 1)
        across = copy_of(source, block, cut, partner, 2)
        return left, right, across

    for cut in range(len(cuts)):
        left, right, across = moves(me, cut, feat)
        pl.when(has_left)(left.start)
        pl.when(has_right)(right.start)
        across.start()
    for load in loads:
        load.start()

    def project(rows_in, block):
        value_t = lax.dot_general(
            w_value_t[...], rows_in, (((1,), (1,)), ((), ())), preferred_element_type=F32
        )
        values[block, :, 0:tokens] = (value_t + shift_t[:, 0:1]).astype(BF16).astype(F32)

    def stage(distance, cut):
        before, after = me - 2 * distance, me + 2 * distance

        @pl.when(mine_z >= distance)
        def _():
            left, right, across = moves(before, cut)
            across.wait_recv()
            pl.when(has_right)(right.start)
            across.start()

        @pl.when(mine_z + distance < line)
        def _():
            left, right, across = moves(after, cut)
            across.wait_recv()
            pl.when(has_left)(left.start)
            across.start()

        if cut == len(cuts) - 1:
            pl.when(mine_z >= distance)(lambda: project(gathered[before], before))
            pl.when(mine_z + distance < line)(lambda: project(gathered[after], after))

    def arrive(block):
        for cut in range(len(cuts)):
            moves(block, cut)[2].wait_recv()
        project(gathered[block], block)

    def finish(block, came_left, came_right, own=False):
        for cut in range(len(cuts)):
            left, right, across = moves(block, cut, feat if own else None)
            if own or came_right:
                pl.when(has_left)(left.wait_send)
            if own or came_left:
                pl.when(has_right)(right.wait_send)
            across.wait_send()

    for load in loads[:4]:
        load.wait()
    w_value_t[...] = jnp.transpose(w_value[...].astype(F32)).astype(BF16)
    shift_t[...] = jnp.transpose(jnp.broadcast_to(b_value[...], (LANES, model)))

    def turned(block):
        tail = jnp.zeros((padded - tokens, block.shape[1]), F32)
        return jnp.transpose(jnp.concatenate([block, tail], axis=0))

    corner_t = turned(corners[...].astype(F32))
    group_t[...] = jnp.floor((corner_t + 0.5) * (1.0 / STRIDE))
    place_t[...] = corner_t
    bil_t[...] = turned(bilinear[...])
    att_t[...] = turned(attention[...])
    for level in range(LEVELS):
        flats[level][...] = jnp.zeros(flats[level].shape, F32)

    iota = lax.broadcasted_iota(jnp.int32, (LANES, padded), 0).astype(F32)

    def point_weights(point):
        share = att_t[pl.ds(point, 1), :]
        return [
            (share * bil_t[pl.ds(point * 4 + corner, 1), :]).astype(BF16).astype(F32)
            for corner in range(4)
        ]

    def build(head, carry):
        for slot, level in enumerate(windowed):
            for which in range(POINTS):
                point = (head * LEVELS + level) * POINTS + which
                place = place_t[pl.ds(point * 4, 1), :] - STRIDE * group_t[pl.ds(point * 4, 1), :]
                top, bottom = one_hot_pair(iota, place, point_weights(point))
                hot[head, slot * POINTS + which, 0:LANES, :] = top.astype(BF16)
                hot[head, slot * POINTS + which, LANES:, :] = bottom.astype(BF16)
        top_sum = jnp.zeros((LANES, padded), F32)
        bottom_sum = jnp.zeros((LANES, padded), F32)
        for level in merged:
            for which in range(POINTS):
                point = (head * LEVELS + level) * POINTS + which
                place = place_t[pl.ds(point * 4, 1), :] + float(merged[level])
                top, bottom = one_hot_pair(iota, place, point_weights(point))
                top_sum += top
                bottom_sum += bottom
        hot_merged[head, 0:LANES, :] = top_sum.astype(BF16)
        hot_merged[head, LANES:, :] = bottom_sum.astype(BF16)
        return carry

    stages = [(distance, cut) for distance in range(1, line) for cut in range(len(cuts))]
    done = 0
    for number, entry in enumerate(stages):
        upto = min(HEADS, BUILT[min(number, len(BUILT) - 1)])
        if upto > done:
            lax.fori_loop(done, upto, build, 0)
            done = upto
        if number == 0:
            project(feat[...], me)
        stage(*entry)
    if done < HEADS:
        lax.fori_loop(done, HEADS, build, 0)
    arrive(partner)
    for distance in range(1, line):
        pl.when(mine_z >= distance)(functools.partial(arrive, partner - 2 * distance))
        pl.when(mine_z + distance < line)(functools.partial(arrive, partner + 2 * distance))

    for band in range(bands):
        value_t = values[band]
        for level in range(LEVELS):
            count = rows[level]
            flats[level][:, band * count : (band + 1) * count] = value_t[
                :, starts[level] : starts[level] + count
            ]

    for level in windowed:
        for group in range(groups[level]):
            base = STRIDE * group
            top = flats[level][:, base : base + LANES].astype(BF16)
            under = base + widths[level]
            bottom = flats[level][:, under : under + LANES].astype(BF16)
            for head in range(HEADS):
                part = slice(head * head_dim, (head + 1) * head_dim)
                into = slice(group * head_dim, (group + 1) * head_dim)
                tables[level][head, into, 0:LANES] = top[part, :]
                tables[level][head, into, LANES:] = bottom[part, :]
    lane = lax.broadcasted_iota(jnp.int32, (1, LANES), 1)
    top = jnp.zeros((model, LANES), F32)
    bottom = jnp.zeros((model, LANES), F32)
    for level, begin in merged.items():
        inside = (lane >= begin) & (lane < begin + lengths[level])
        piece = flats[level][:, 0:LANES]
        top += jnp.where(inside, pltpu.roll(piece, begin, 1), 0.0)
        bottom += jnp.where(
            inside, pltpu.roll(piece, (begin - widths[level]) % LANES, 1), 0.0
        )
    for head in range(HEADS):
        part = slice(head * head_dim, (head + 1) * head_dim)
        table_merged[head, :, 0:LANES] = top[part, :].astype(BF16)
        table_merged[head, :, LANES:] = bottom[part, :].astype(BF16)

    def blend(head, carry):
        total = jnp.dot(table_merged[head], hot_merged[head], preferred_element_type=F32)
        for slot, level in enumerate(windowed):
            for which in range(POINTS):
                point = (head * LEVELS + level) * POINTS + which
                mine = group_t[pl.ds(point * 4, 1), :]
                picked = jnp.dot(
                    tables[level][head],
                    hot[head, slot * POINTS + which],
                    preferred_element_type=F32,
                )
                for group in range(groups[level]):
                    total += jnp.where(
                        mine == float(group),
                        picked[group * head_dim : (group + 1) * head_dim, :],
                        0.0,
                    )
        samp_t[pl.ds(pl.multiple_of(head * head_dim, head_dim), head_dim), :] = total
        return carry

    lax.fori_loop(0, HEADS, blend, 0)

    for load in loads[4:]:
        load.wait()
    sampled = jnp.transpose(samp_t[...])[0:tokens, :].astype(BF16)
    attended = jnp.dot(sampled, w_out[...], preferred_element_type=F32) + b_out[...]
    middle = norm(feat[...].astype(F32) + attended, gain1[...], bias1[...]).astype(BF16)
    hidden = jnp.maximum(
        jnp.dot(middle, w_in[...], preferred_element_type=F32) + b_in[...], 0.0
    ).astype(BF16)
    result = (
        middle.astype(F32)
        + jnp.dot(hidden, w_ff[...], preferred_element_type=F32)
        + b_ff[...]
    )
    out[...] = norm(result, gain2[...], bias2[...]).astype(BF16)
    finish(me, False, False, own=True)
    for distance in range(1, line):
        pl.when(mine_z >= distance)(
            functools.partial(finish, me - 2 * distance, True, False)
        )
        pl.when(mine_z + distance < line)(
            functools.partial(finish, me + 2 * distance, False, True)
        )


def body(bands, *args):
    feat, corners = args[0], args[1]
    tokens, model = feat.shape
    padded = -(-tokens // LANES) * LANES
    rows, starts, widths, lengths, merged, windowed, groups = plan(bands)
    head_dim = model // HEADS
    samples = corners.shape[1]
    operands = [
        argument.reshape(1, -1) if argument.ndim == 1 else argument for argument in args
    ]
    anywhere = {1, 2, 3, 4, 6, 10, 12}
    cuts = -(-tokens // CHUNK)
    specs = [
        pl.BlockSpec(memory_space=pl.ANY if number in anywhere else pltpu.VMEM)
        for number in range(len(operands))
    ]
    flat_shapes = [
        pltpu.VMEM(
            (model, flat_lanes(lengths[level], widths[level], groups.get(level, 1))), F32
        )
        for level in range(LEVELS)
    ]
    table_shapes = [
        pltpu.VMEM((HEADS, groups[level] * head_dim, 2 * LANES), BF16) for level in windowed
    ]
    scratch = [
        pltpu.VMEM((bands, tokens, model), BF16),
        pltpu.VMEM((bands, model, padded), F32),
        pltpu.VMEM(args[1].shape, jnp.int32),
        pltpu.VMEM(args[2].shape, F32),
        pltpu.VMEM(args[3].shape, F32),
        pltpu.VMEM(args[4].shape, BF16),
        pltpu.VMEM(args[4].shape, BF16),
        pltpu.VMEM((model, LANES), F32),
        pltpu.VMEM((samples, padded), F32),
        pltpu.VMEM((samples, padded), F32),
        pltpu.VMEM((samples, padded), F32),
        pltpu.VMEM((samples // 4, padded), F32),
        pltpu.VMEM((HEADS, len(windowed) * POINTS, 2 * LANES, padded), BF16),
        pltpu.VMEM((HEADS, 2 * LANES, padded), BF16),
        pltpu.VMEM((HEADS, head_dim, 2 * LANES), BF16),
        pltpu.VMEM((model, padded), F32),
        pltpu.VMEM(args[6].shape, BF16),
        pltpu.VMEM(args[10].shape, BF16),
        pltpu.VMEM(args[12].shape, BF16),
        pltpu.SemaphoreType.DMA((3, bands, cuts)),
        pltpu.SemaphoreType.DMA((bands, cuts)),
        pltpu.SemaphoreType.DMA((len(anywhere),)),
    ] + flat_shapes + table_shapes
    return pl.pallas_call(
        functools.partial(kernel, bands),
        out_shape=jax.ShapeDtypeStruct((tokens, model), BF16),
        in_specs=specs,
        out_specs=pl.BlockSpec(memory_space=pltpu.VMEM),
        scratch_shapes=scratch,
        compiler_params=pltpu.CompilerParams(
            collective_id=0, has_side_effects=True, vmem_limit_bytes=60 * 1024 * 1024
        ),
        name="layer",
    )(*operands)


def solution(mesh):
    split = P(("dp", "band"), None)
    in_specs = (split,) * 4 + (P(),) * 12
    return jax.shard_map(
        functools.partial(body, mesh.shape["band"]),
        mesh=mesh,
        in_specs=in_specs,
        out_specs=split,
        check_vma=False,
    )
```
